32 devices in a mesh: terms: 32 (over z, y, x, core).
Axes of the slice: x: 2, y: 2, z: 4, core: 2. Of those that a mesh axis runs over, the one named last changes fastest.
Arguments:
- psi_init: float32 [512, 4, 4, 512], replicated
- left_env: bfloat16 [96, 512, 512], P('terms')
- op_pair: bfloat16 [96, 16, 16], P('terms')
- right_env: bfloat16 [96, 512, 512], P('terms')
Outputs:
- output 1: float32 [7, 512, 4, 4, 512], P(None, 'terms')
- output 2: float32 [6], replicated
- output 3: float32 [6], replicated
All inputs are finite; a program needn't handle non-finite values.
Results may differ from the reference program's by a relative error of at most 0.0168708.
Values are sent between devices in bfloat16 or wider.
A program may use at most 1 GiB of HBM per device.

```python
import jax
import jax.numpy as jnp
from jax import lax

BOND = 512
PHYS = 4
TERMS = 96
KRYLOV_STEPS = 6


def symmetric_stack(key_in, count, size):
    gauss_draws = jax.random.normal(key_in, (count, size, size), jnp.float32)
    return (gauss_draws + jnp.swapaxes(gauss_draws, 1, 2)) * (0.5 * (2.0 * size) ** -0.5)


def setup_inputs(seed: int = 0) -> dict:
    root_key = jax.random.key(seed)
    key_psi, key_left, key_pair, key_right, key_shift = jax.random.split(root_key, 5)
    pair_dim = PHYS * PHYS
    shifts = 0.5 * jax.random.normal(key_shift, (3, TERMS), jnp.float32)
    eye_bond = jnp.eye(BOND, dtype=jnp.float32)
    eye_pair = jnp.eye(pair_dim, dtype=jnp.float32)
    term_scale = 2.0 * TERMS ** -0.5
    psi_init = jax.random.normal(key_psi, (BOND, PHYS, PHYS, BOND), jnp.float32)
    left_env = term_scale * (symmetric_stack(key_left, TERMS, BOND) + shifts[0][:, None, None] * eye_bond)
    op_pair = symmetric_stack(key_pair, TERMS, pair_dim) + shifts[1][:, None, None] * eye_pair
    right_env = symmetric_stack(key_right, TERMS, BOND) + shifts[2][:, None, None] * eye_bond
    return {'psi_init': psi_init, 'left_env': left_env.astype(jnp.bfloat16), 'op_pair': op_pair.astype(jnp.bfloat16), 'right_env': right_env.astype(jnp.bfloat16)}


def reference(psi_init, left_env, op_pair, right_env):
    pair_dim = PHYS * PHYS
    elem_count = BOND * pair_dim * BOND

    def apply_terms(vector):
        vector_low = vector.astype(jnp.bfloat16).reshape(BOND * pair_dim, BOND)

        def one_term(sigma_sum, term_mats):
            left_mat, pair_mat, right_mat = term_mats
            y_part = jnp.dot(vector_low, right_mat.T, preferred_element_type=jnp.float32)
            y_part = y_part.astype(jnp.bfloat16).reshape(BOND, pair_dim, BOND)
            z_part = jnp.einsum('qp,apb->aqb', pair_mat.astype(jnp.float32), y_part.astype(jnp.float32))
            z_part = z_part.astype(jnp.bfloat16).reshape(BOND, pair_dim * BOND)
            term_out = jnp.dot(left_mat, z_part, preferred_element_type=jnp.float32)
            return sigma_sum + term_out.reshape(BOND, pair_dim, BOND), None

        sigma_sum, _ = lax.scan(one_term, jnp.zeros((BOND, pair_dim, BOND), jnp.float32), (left_env, op_pair, right_env))
        return sigma_sum

    vector = psi_init.reshape(BOND, pair_dim, BOND)
    vector = vector / jnp.sqrt(jnp.sum(vector * vector) / elem_count)
    vectors = [vector]
    alphas = []
    betas = []
    prev_vector = vector
    for step_idx in range(KRYLOV_STEPS):
        sigma_sum = apply_terms(vector)
        alpha_val = jnp.sum(sigma_sum * vector) / elem_count
        residual = sigma_sum - alpha_val * vector
        if step_idx > 0:
            residual = residual - betas[-1] * prev_vector
        beta_val = jnp.sqrt(jnp.sum(residual * residual) / elem_count)
        prev_vector = vector
        vector = residual / beta_val
        vectors.append(vector)
        alphas.append(alpha_val)
        betas.append(beta_val)
    krylov_vectors = jnp.stack(vectors).reshape(KRYLOV_STEPS + 1, BOND, PHYS, PHYS, BOND)
    return krylov_vectors, jnp.stack(alphas), jnp.stack(betas)
```

```python
import functools

import jax
import jax.numpy as jnp
from jax import lax
from jax.experimental import pallas as pl
from jax.experimental.pallas import tpu as pltpu
from jax.sharding import PartitionSpec as P

KRYLOV_STEPS = 6
MESH = pl.DeviceIdType.MESH
NDEV = 32
NT = 96
NC = 4
GP = 4
GR = 16


def coords(me):
    z = me // 8
    return z // 2, lax.rem(z, 2), lax.rem(me // 4, 2), lax.rem(me // 2, 2), lax.rem(me, 2)


def dev_id(zh, zl, y, x, c):
    return zh * 16 + zl * 8 + y * 4 + x * 2 + c


def kernel(elem_count, vb0_ref, lh_ref, kr_ref, rr_ref, v0_ref, out_ref, alpha_ref, beta_ref,
           vbuf, vsend, xs, sacc, rsr, vs, arr, bsc,
           in_sem, out_sem, rs_send, rs_recv, ar_send, ar_recv, aa_send, aa_recv, ag_send, ag_recv):
    f32, bf16 = jnp.float32, jnp.bfloat16
    me = lax.axis_index('terms')
    zh, zl, y, x, c = coords(me)
    role = 2 * zl + x
    unit = 4 * zh + 2 * y + c
    inv_n = 1.0 / elem_count
    rs_dev = [dev_id(zh, zl, y, 1 - x, c), dev_id(zh, 1 - zl, y, x, c), dev_id(zh, 1 - zl, y, 1 - x, c)]
    rs_role = [2 * zl + (1 - x), 2 * (1 - zl) + x, 2 * (1 - zl) + (1 - x), role]
    dev_z = dev_id(1 - zh, zl, y, x, c)
    dev_y = dev_id(zh, zl, 1 - y, x, c)
    dev_c = dev_id(zh, zl, y, x, 1 - c)
    own_rows = pl.ds(pl.multiple_of(role * 16, 16), 16)
    ppc = 8 // NC

    def aa_copy(ch, i):
        pps = pl.ds(ch * ppc, ppc)
        return pltpu.make_async_remote_copy(
            src_ref=vsend.at[rs_role[i], pps], dst_ref=vbuf.at[unit, pps, own_rows],
            send_sem=aa_send.at[ch, i], recv_sem=aa_recv.at[ch, i], device_id=(rs_dev[i],), device_id_type=MESH)

    def ag_copy(ch, slot, u, dev):
        pps = pl.ds(ch * ppc, ppc)
        return pltpu.make_async_remote_copy(
            src_ref=vbuf.at[u, pps], dst_ref=vbuf.at[u, pps],
            send_sem=ag_send.at[ch, slot], recv_sem=ag_recv.at[ch, u], device_id=(dev,), device_id_type=MESH)

    unit_z = 4 * (1 - zh) + 2 * y + c
    unit_y = 4 * zh + 2 * (1 - y) + c
    unit_zy = 4 * (1 - zh) + 2 * (1 - y) + c
    sends = [(0, unit, dev_z), (1, unit, dev_y), (2, unit_z, dev_y),
             (3, unit, dev_c), (4, unit_z, dev_c), (5, unit_y, dev_c), (6, unit_zy, dev_c)]

    def start(ch, slots):
        for s in slots:
            ag_copy(ch, *sends[s]).start()

    def recv(ch, u):
        ag_copy(ch, 0, u, dev_c).wait_recv()

    def stage_a(ch):
        for i in range(3):
            aa_copy(ch, i).wait_recv()
        start(ch, (0, 1, 3))

    def stage_z(ch):
        recv(ch, unit_z)
        start(ch, (2, 4))

    def stage_y(ch):
        recv(ch, unit_y)
        start(ch, (5,))
        recv(ch, unit_zy)
        start(ch, (6,))

    def stage_c(ch):
        for a in range(2):
            for b in range(2):
                recv(ch, 4 * a + 2 * b + (1 - c))

    def left_chunk(ch):
        def body(i, _):
            pp = ch * ppc + i // 4
            ac = lax.rem(i, 4)
            slab = jnp.where(ac == 0, rs_role[0], jnp.where(ac == 1, rs_role[1], jnp.where(ac == 2, rs_role[2], role)))
            rhs = vbuf[:, pp].reshape(512, 256)
            res = jnp.dot(lh_ref[slab], rhs, preferred_element_type=f32).astype(bf16).reshape(NT, 16, 256)
            ap = ac // 2

            @pl.when(lax.rem(ac, 2) == 0)
            def _():
                xs[ap, :, 2 * pp, :, 0:128] = res[:, :, 0:128]
                xs[ap, :, 2 * pp + 1, :, 0:128] = res[:, :, 128:256]

            @pl.when(lax.rem(ac, 2) == 1)
            def _():
                xs[ap, :, 2 * pp, :, 128:256] = res[:, :, 0:128]
                xs[ap, :, 2 * pp + 1, :, 128:256] = res[:, :, 128:256]
            return 0
        lax.fori_loop(0, ppc * 4, body, 0)

    def pair_phase(ap):
        def body(i, _):
            for g in range(GP):
                k = i * GP + g
                zval = jnp.dot(kr_ref[k], xs[ap, k].reshape(256, 256), preferred_element_type=f32).astype(bf16)
                xs[ap, k] = zval.reshape(16, 16, 256)
            return 0
        lax.fori_loop(0, NT // GP, body, 0)

    def right_phase(ap, h, dst):
        def piece(k0):
            lhs = jnp.concatenate([xs[ap, k0 + g].reshape(256, 256)[:, h * 128:(h + 1) * 128] for g in range(GR)], axis=1)
            rhs = rr_ref[pl.ds(k0, GR)].reshape(GR * 128, 512)
            return jnp.dot(lhs, rhs, preferred_element_type=f32).reshape(16, 16, 512)
        sacc[dst] = jnp.zeros((16, 16, 512), f32)

        def body(i, _):
            sacc[dst] += piece(i * GR)
            return 0
        lax.fori_loop(0, NT // GR, body, 0)

    def rs_copy(i):
        return pltpu.make_async_remote_copy(
            src_ref=sacc.at[i], dst_ref=rsr.at[i], send_sem=rs_send.at[i], recv_sem=rs_recv.at[i],
            device_id=(rs_dev[i],), device_id_type=MESH)

    def total(val):
        return jnp.sum(jnp.sum(val, axis=0, keepdims=True), axis=1, keepdims=True)

    def out_copy(slot, j):
        return pltpu.make_async_copy(vs.at[slot], out_ref.at[j], out_sem)

    loads = [pltpu.make_async_copy(v0_ref, vs.at[0], in_sem.at[0]), pltpu.make_async_copy(vb0_ref, vbuf, in_sem.at[1])]
    for cp in loads:
        cp.start()
    vs[2] = jnp.zeros((16, 16, 512), f32)
    bsc[...] = jnp.zeros((8, 128), f32)
    for cp in loads:
        cp.wait()
    out_copy(0, 0).start()

    def step(j, _):
        cur = lax.rem(j, 3)
        nxt = lax.rem(j + 1, 3)
        prv = lax.rem(j + 2, 3)
        par = lax.rem(j, 2)

        @pl.when(j > 0)
        def _():
            for t in range(NC + 2):
                if t < NC:
                    stage_a(t)
                if 0 <= t - 1 < NC:
                    stage_z(t - 1)
                if 0 <= t - 2 < NC:
                    stage_y(t - 2)

        for ch in range(NC):
            @pl.when(j > 0)
            def _():
                stage_c(ch)
            left_chunk(ch)

        @pl.when(j > 0)
        def _():
            for ch in range(NC):
                for i in range(3):
                    aa_copy(ch, i).wait_send()
                for s in sends:
                    ag_copy(ch, *s).wait_send()

        pair_phase(0)
        right_phase(0, 0, 0)
        rs_copy(0).start()
        right_phase(0, 1, 1)
        rs_copy(1).start()
        pair_phase(1)
        right_phase(1, 0, 2)
        rs_copy(2).start()
        right_phase(1, 1, 3)
        out_copy(cur, j).wait()
        for i in range(3):
            rs_copy(i).wait()

        beta_prev = bsc[0:1, 0:1]

        def pass1(p, acc):
            s1, sb, vv = acc
            w = ((sacc[3, p] + rsr[0, p]) + (rsr[1, p] + rsr[2, p]))
            v = vs[cur, p]
            sacc[3, p] = w
            return s1 + w * v, sb + (w - beta_prev * vs[prv, p]) * v, vv + v * v
        zero = jnp.zeros((16, 512), f32)
        s1, sb, vv = lax.fori_loop(0, 16, pass1, (zero, zero, zero))
        s1, sb, vv = total(s1), total(sb), total(vv)
        a_loc = jnp.where(vv > 1e-6, sb / jnp.where(vv > 1e-6, vv, 1.0), 0.0)

        def pass2(p, acc):
            uu, uv = acc
            v = vs[cur, p]
            u = sacc[3, p] - beta_prev * vs[prv, p] - a_loc * v
            return uu + u * u, uv + u * v
        uu, uv = lax.fori_loop(0, 16, pass2, (zero, zero))
        uu, uv = total(uu), total(uv)
        row = lax.broadcasted_iota(jnp.int32, (8, 128), 0)
        msg = jnp.where(row == 0, s1, jnp.where(row == 1, a_loc, jnp.where(row == 2, uu, jnp.where(row == 3, uv, vv))))
        arr[par, me] = msg

        def ar_copy(i):
            return pltpu.make_async_remote_copy(
                src_ref=arr.at[par, me], dst_ref=arr.at[par, me], send_sem=ar_send, recv_sem=ar_recv,
                device_id=(lax.rem(me + i, NDEV),), device_id_type=MESH)

        def send_msg(i, _):
            ar_copy(i).start()
            return 0
        lax.fori_loop(1, NDEV, send_msg, 0)
        pltpu.make_async_copy(arr.at[par, pl.ds(0, NDEV - 1)], arr.at[par, pl.ds(0, NDEV - 1)], ar_recv).wait()
        pltpu.make_async_copy(arr.at[par, pl.ds(0, NDEV - 1)], arr.at[par, pl.ds(0, NDEV - 1)], ar_send).wait()
        alpha = jnp.sum(arr[par, :, 0], axis=0, keepdims=True) * inv_n
        delta = alpha - arr[par, :, 1]
        rest = arr[par, :, 2] + delta * (delta * arr[par, :, 4] - 2.0 * arr[par, :, 3])
        beta = jnp.sqrt(jnp.sum(rest, axis=0, keepdims=True) * inv_n)
        alpha_ref[pl.ds(j, 1), :] = alpha
        beta_ref[pl.ds(j, 1), :] = beta
        bsc[0:1, :] = beta
        alpha11 = alpha[:, 0:1]
        beta11 = beta[:, 0:1]

        def update(p, _):
            vs[nxt, p] = (sacc[3, p] - alpha11 * vs[cur, p] - beta_prev * vs[prv, p]) / beta11
            return 0
        lax.fori_loop(0, 16, update, 0)
        out_copy(nxt, j + 1).start()

        @pl.when(j < KRYLOV_STEPS - 1)
        def _():
            for ch in range(NC):
                def fill(pp, _):
                    even = vs[nxt, 2 * pp].astype(bf16)
                    odd = vs[nxt, 2 * pp + 1].astype(bf16)
                    for r in range(4):
                        vsend[r, pp, :, 0:128] = even[:, r * 128:(r + 1) * 128]
                        vsend[r, pp, :, 128:256] = odd[:, r * 128:(r + 1) * 128]
                    vbuf[unit, pp, own_rows, :] = vsend[role, pp]
                    return 0
                lax.fori_loop(ch * ppc, (ch + 1) * ppc, fill, 0)
                for i in range(3):
                    aa_copy(ch, i).start()
        return 0

    lax.fori_loop(0, KRYLOV_STEPS, step, 0)
    out_copy(KRYLOV_STEPS % 3, KRYLOV_STEPS).wait()


def run_kernel(elem_count, vb0, lh, kron, rr, v0):
    f32, bf16 = jnp.float32, jnp.bfloat16
    vm = pl.BlockSpec(memory_space=pltpu.VMEM)
    dma = pltpu.SemaphoreType.DMA
    return pl.pallas_call(
        functools.partial(kernel, elem_count),
        out_shape=(jax.ShapeDtypeStruct((KRYLOV_STEPS + 1, 16, 16, 512), f32),
                   jax.ShapeDtypeStruct((8, 128), f32), jax.ShapeDtypeStruct((8, 128), f32)),
        in_specs=[pl.BlockSpec(memory_space=pl.ANY), vm, vm, vm, pl.BlockSpec(memory_space=pl.ANY)],
        out_specs=(pl.BlockSpec(memory_space=pl.ANY), vm, vm),
        scratch_shapes=[
            pltpu.VMEM((8, 8, 64, 256), bf16),
            pltpu.VMEM((4, 8, 16, 256), bf16),
            pltpu.VMEM((2, NT, 16, 16, 256), bf16),
            pltpu.VMEM((4, 16, 16, 512), f32),
            pltpu.VMEM((3, 16, 16, 512), f32),
            pltpu.VMEM((3, 16, 16, 512), f32),
            pltpu.VMEM((2, NDEV, 8, 128), f32),
            pltpu.VMEM((8, 128), f32),
            dma((2,)), dma, dma((3,)), dma((3,)), dma, dma, dma((NC, 3)), dma((NC, 3)), dma((NC, 7)), dma((NC, 8)),
        ],
        compiler_params=pltpu.CompilerParams(has_side_effects=True, vmem_limit_bytes=67043328),
    )(vb0, lh, kron, rr, v0)


def solution(mesh):

    def index(zh, zl, y, x, c):
        return zh * 16 + zl * 8 + y * 4 + x * 2 + c
    role_groups = [[index(zh, zl, y, x, c) for zl in (0, 1) for x in (0, 1)]
                   for zh in (0, 1) for y in (0, 1) for c in (0, 1)]
    unit_groups = [[index(zh, zl, y, x, c) for zh in (0, 1) for y in (0, 1) for c in (0, 1)]
                   for zl in (0, 1) for x in (0, 1)]

    def local_run(psi_init, left_env, op_pair, right_env):
        f32, bf16 = jnp.float32, jnp.bfloat16
        me = lax.axis_index('terms')
        zh, zl, y, x, c = coords(me)
        role = 2 * zl + x
        elem_count = psi_init.size
        psi = psi_init.reshape(512, 16, 512)
        norm = jnp.sqrt(jnp.sum(psi * psi) / elem_count)
        cols = lax.dynamic_slice_in_dim(psi, role * 128, 128, 2)
        vb0 = (cols / norm).astype(bf16).reshape(2, 2, 2, 2, 2, 16, 8, 2, 128)
        vb0 = vb0.transpose(0, 2, 4, 6, 1, 3, 5, 7, 8).reshape(8, 8, 64, 256)
        v0 = (lax.dynamic_slice_in_dim(psi, me * 16, 16, 0) / norm).transpose(1, 0, 2)

        rr = lax.all_to_all(right_env, 'terms', 1, 0, tiled=True, axis_index_groups=role_groups)
        rr = lax.all_gather(rr, 'terms', axis=0, tiled=True, axis_index_groups=unit_groups)

        lp = left_env.reshape(3, 2, 2, 2, 2, 2, 16, 2, 2, 2, 2, 2, 16)
        lp = lp.transpose(0, 1, 3, 5, 2, 4, 6, 7, 9, 11, 8, 10, 12).reshape(3, 512, 512)
        lp = lax.all_gather(lp, 'terms', axis=0, tiled=True, axis_index_groups=role_groups)
        lp = lax.all_to_all(lp, 'terms', 1, 0, tiled=True, axis_index_groups=unit_groups)
        lh = lp.reshape(NT, 4, 16, 512).transpose(1, 0, 2, 3).reshape(4, NT * 16, 512)

        wk = lax.all_gather(op_pair, 'terms', axis=0, tiled=True).reshape(2, 2, 2, 2, 2, 3, 16, 16)
        wk = wk.transpose(0, 2, 4, 1, 3, 5, 6, 7).reshape(NT, 16, 16)
        eye = jnp.eye(16, dtype=bf16)
        kron = (wk[:, :, None, :, None] * eye[None, None, :, None, :]).reshape(NT, 256, 256)

        out, alpha, beta = run_kernel(elem_count, vb0, lh, kron, rr, v0)
        vecs = out.transpose(0, 2, 1, 3).reshape(KRYLOV_STEPS + 1, 16, 4, 4, 512)
        return vecs, alpha[:KRYLOV_STEPS, 0], beta[:KRYLOV_STEPS, 0]

    return jax.shard_map(local_run, mesh=mesh, in_specs=(P(), P('terms'), P('terms'), P('terms')),
                         out_specs=(P(None, 'terms'), P(), P()), check_vma=False)
```

```python
import functools

import jax
import jax.numpy as jnp
from jax import lax
from jax.experimental import pallas as pl
from jax.experimental.pallas import tpu as pltpu
from jax.sharding import PartitionSpec as P

KRYLOV_STEPS = 6
MESH = pl.DeviceIdType.MESH
NDEV = 32
NT = 96
NC = 4
GP = 16
GR = 32


def coords(me):
    z = me // 8
    return z // 2, lax.rem(z, 2), lax.rem(me // 4, 2), lax.rem(me // 2, 2), lax.rem(me, 2)


def dev_id(zh, zl, y, x, c):
    return zh * 16 + zl * 8 + y * 4 + x * 2 + c


def kernel(elem_count, vb0_ref, left_ref, wx_ref, right_ref, v0_ref, out_ref, alpha_ref, beta_ref,
           lh_ref, kr_ref, rr_ref, vbuf, vsend, xs, sacc, rsr, vs, arr, bsc,
           in_sem, w_send, w_recv, r1_send, r1_recv, rg_send, rg_recv, l1_send, l1_recv, l2_send, l2_recv,
           out_sem, rs_send, rs_recv, ar_send, ar_recv, aa_send, aa_recv, ag_send, ag_recv):
    f32, bf16 = jnp.float32, jnp.bfloat16
    me = lax.axis_index('terms')
    zh, zl, y, x, c = coords(me)
    role = 2 * zl + x
    unit = 4 * zh + 2 * y + c
    inv_n = 1.0 / elem_count
    rs_dev = [dev_id(zh, zl, y, 1 - x, c), dev_id(zh, 1 - zl, y, x, c), dev_id(zh, 1 - zl, y, 1 - x, c)]
    rs_role = [2 * zl + (1 - x), 2 * (1 - zl) + x, 2 * (1 - zl) + (1 - x), role]
    dev_z = dev_id(1 - zh, zl, y, x, c)
    dev_y = dev_id(zh, zl, 1 - y, x, c)
    dev_c = dev_id(zh, zl, y, x, 1 - c)
    kpos = 4 * unit + role
    ppc = 8 // NC

    def aa_copy(ch, i):
        pps = pl.ds(ch * ppc, ppc)
        return pltpu.make_async_remote_copy(
            src_ref=vsend.at[rs_role[i], pps], dst_ref=vbuf.at[zh, zl, y, x, c, pps],
            send_sem=aa_send.at[ch, i], recv_sem=aa_recv.at[ch, i], device_id=(rs_dev[i],), device_id_type=MESH)

    def ag_copy(ch, slot, u, dev):
        block = vbuf.at[u // 4, :, lax.rem(u // 2, 2), :, lax.rem(u, 2), pl.ds(ch * ppc, ppc)]
        return pltpu.make_async_remote_copy(
            src_ref=block, dst_ref=block,
            send_sem=ag_send.at[ch, slot], recv_sem=ag_recv.at[ch, u], device_id=(dev,), device_id_type=MESH)

    unit_z = 4 * (1 - zh) + 2 * y + c
    unit_y = 4 * zh + 2 * (1 - y) + c
    unit_zy = 4 * (1 - zh) + 2 * (1 - y) + c
    sends = [(0, unit, dev_z), (1, unit, dev_y), (2, unit_z, dev_y),
             (3, unit, dev_c), (4, unit_z, dev_c), (5, unit_y, dev_c), (6, unit_zy, dev_c)]

    def start(ch, slots):
        for s in slots:
            ag_copy(ch, *sends[s]).start()

    def recv(ch, u):
        ag_copy(ch, 0, u, dev_c).wait_recv()

    def stage_a(ch):
        for i in range(3):
            aa_copy(ch, i).wait_recv()
        start(ch, (0, 1, 3))

    def stage_z(ch):
        recv(ch, unit_z)
        start(ch, (2, 4))

    def stage_y(ch):
        recv(ch, unit_y)
        start(ch, (5,))
        recv(ch, unit_zy)
        start(ch, (6,))

    def stage_c(ch):
        for a in range(2):
            for b in range(2):
                recv(ch, 4 * a + 2 * b + (1 - c))

    def left_part(pp):
        def body(ap, _):
            rhs = vbuf[:, :, :, :, :, pp].reshape(512, 256)
            for h in range(2):
                slab = jnp.where(ap == 0, rs_role[h], rs_role[2 + h])
                res = jnp.dot(lh_ref[slab].reshape(NT * 16, 512), rhs, preferred_element_type=f32)
                res = res.astype(bf16).reshape(NT, 16, 256)
                xs[ap, :, 2 * pp, :, h * 128:(h + 1) * 128] = res[:, :, 0:128]
                xs[ap, :, 2 * pp + 1, :, h * 128:(h + 1) * 128] = res[:, :, 128:256]
            return 0
        lax.fori_loop(0, 2, body, 0)

    def pair_phase(ap):
        def body(i, _):
            for g in range(GP):
                k = i * GP + g
                zval = jnp.dot(kr_ref[k], xs[ap, k].reshape(256, 256), preferred_element_type=f32).astype(bf16)
                xs[ap, k] = zval.reshape(16, 16, 256)
            return 0
        lax.fori_loop(0, NT // GP, body, 0)

    def right_phase(ap, h, dst):
        def piece(k0):
            lhs = jnp.concatenate([xs[ap, k0 + g].reshape(256, 256)[:, h * 128:(h + 1) * 128] for g in range(GR)], axis=1)
            rhs = rr_ref[pl.ds(k0, GR)].reshape(GR * 128, 512)
            return jnp.dot(lhs, rhs, preferred_element_type=f32).reshape(16, 16, 512)
        sacc[dst] = jnp.zeros((16, 16, 512), f32)

        def body(i, _):
            sacc[dst] += piece(i * GR)
            return 0
        lax.fori_loop(0, NT // GR, body, 0)

    def rs_copy(i):
        return pltpu.make_async_remote_copy(
            src_ref=sacc.at[i], dst_ref=rsr.at[i], send_sem=rs_send.at[i], recv_sem=rs_recv.at[i],
            device_id=(rs_dev[i],), device_id_type=MESH)

    def total(val):
        return jnp.sum(jnp.sum(val, axis=0, keepdims=True), axis=1, keepdims=True)

    def out_copy(slot, j):
        return pltpu.make_async_copy(vs.at[slot], out_ref.at[j], out_sem)

    order = [role] + rs_role[:3]

    def r_rows(u, ro):
        return pl.ds(12 * u + 3 * ro, 3)

    def r1_copy(i):
        return pltpu.make_async_remote_copy(
            src_ref=right_ref.at[:, pl.ds(pl.multiple_of(128 * rs_role[i], 128), 128)],
            dst_ref=rr_ref.at[r_rows(unit, role)],
            send_sem=r1_send.at[i], recv_sem=r1_recv.at[i], device_id=(rs_dev[i],), device_id_type=MESH)

    def rg_copy(i, slot, u, dev):
        rows = r_rows(u, order[i])
        return pltpu.make_async_remote_copy(
            src_ref=rr_ref.at[rows], dst_ref=rr_ref.at[rows],
            send_sem=rg_send.at[i, slot], recv_sem=rg_recv.at[i, u], device_id=(dev,), device_id_type=MESH)

    def l_rows(d):
        return left_ref.at[:, pl.ds(pl.multiple_of(16 * d, 16), 16)]

    def l1_copies(n):
        uzh, uy, uc = lax.rem(zh + n // 4, 2), lax.rem(y + (n // 2) % 2, 2), lax.rem(c + n % 2, 2)
        dev = dev_id(uzh, zl, uy, x, uc)
        return [pltpu.make_async_remote_copy(
            src_ref=l_rows(dev_id(uzh, r // 2, uy, r % 2, uc)), dst_ref=lh_ref.at[r, unit, role],
            send_sem=l1_send, recv_sem=l1_recv, device_id=(dev,), device_id_type=MESH) for r in range(4)]

    def l2_copy(i):
        return pltpu.make_async_remote_copy(
            src_ref=lh_ref.at[:, :, role], dst_ref=lh_ref.at[:, :, role],
            send_sem=l2_send.at[i], recv_sem=l2_recv.at[i], device_id=(rs_dev[i],), device_id_type=MESH)

    def w_copy(i):
        return pltpu.make_async_remote_copy(
            src_ref=wx_ref, dst_ref=xs.at[1, pl.ds(3 * kpos, 3), 0], send_sem=w_send, recv_sem=w_recv,
            device_id=(lax.rem(me + i, NDEV),), device_id_type=MESH)

    def local_wait(ref, sem):
        pltpu.make_async_copy(ref, ref, sem).wait()

    def gather_operators():
        own_r = pltpu.make_async_copy(
            right_ref.at[:, pl.ds(pl.multiple_of(128 * role, 128), 128)], rr_ref.at[r_rows(unit, role)], in_sem.at[2])
        own_w = pltpu.make_async_copy(wx_ref, xs.at[1, pl.ds(3 * kpos, 3), 0], in_sem.at[3])
        own_l = [pltpu.make_async_copy(l_rows(dev_id(zh, r // 2, y, r % 2, c)), lh_ref.at[r, unit, role],
                                       in_sem.at[4 + r]) for r in range(4)]
        own_r.start()
        own_w.start()
        for cp in own_l:
            cp.start()
        for i in range(3):
            r1_copy(i).start()
        for n in range(1, 8):
            for cp in l1_copies(n):
                cp.start()

        def send_w(i, _):
            w_copy(i).start()
            return 0
        lax.fori_loop(1, NDEV, send_w, 0)

        def r_start(i, slots):
            for k in slots:
                rg_copy(i, *sends[k]).start()

        def r_recv(i, u):
            rg_copy(i, 0, u, dev_c).wait_recv()

        own_r.wait()
        r_start(0, (0, 1, 3))
        for i in range(3):
            r1_copy(i).wait_recv()
            r_start(i + 1, (0, 1, 3))
        for cp in own_l:
            cp.wait()
        l1_part = lh_ref.at[:, pl.ds(0, 7), 0]
        local_wait(l1_part, l1_recv)
        for i in range(3):
            l2_copy(i).start()

        own_w.wait()
        w_part = xs.at[1, pl.ds(0, 93), 0]
        local_wait(w_part, w_recv)
        keep = lax.rem(lax.broadcasted_iota(jnp.int32, (16, 256), 1), 16) == lax.broadcasted_iota(jnp.int32, (16, 256), 0)

        def build(k, _):
            w = xs[1, k, 0].astype(f32)
            for q in range(16):
                kr_ref[k, q * 16:(q + 1) * 16, :] = jnp.where(keep, w[q:q + 1, :], 0.0).astype(bf16)
            return 0
        lax.fori_loop(0, NT, build, 0)

        for t in range(5):
            if t < 4:
                r_recv(t, unit_z)
                r_start(t, (2, 4))
                r_recv(t, unit_y)
                r_start(t, (5,))
            if t >= 1:
                r_recv(t - 1, unit_zy)
                r_start(t - 1, (6,))
        for i in range(3):
            l2_copy(i).wait_recv()
        for i in range(4):
            for a in range(2):
                for b in range(2):
                    r_recv(i, 4 * a + 2 * b + (1 - c))
        for i in range(3):
            r1_copy(i).wait_send()
            l2_copy(i).wait_send()
        local_wait(l1_part, l1_send)
        local_wait(w_part, w_send)
        for i in range(4):
            for k in sends:
                rg_copy(i, *k).wait_send()

    loads = [pltpu.make_async_copy(v0_ref, vs.at[0], in_sem.at[0]), pltpu.make_async_copy(vb0_ref, vbuf, in_sem.at[1])]
    for cp in loads:
        cp.start()
    vs[2] = jnp.zeros((16, 16, 512), f32)
    bsc[...] = jnp.zeros((8, 128), f32)
    gather_operators()
    for cp in loads:
        cp.wait()
    out_copy(0, 0).start()

    def step(j, _):
        cur = lax.rem(j, 3)
        nxt = lax.rem(j + 1, 3)
        prv = lax.rem(j + 2, 3)
        par = lax.rem(j, 2)

        def arrivals(*stages):
            @pl.when(j > 0)
            def _():
                for stage, ch in stages:
                    stage(ch)

        arrivals((stage_a, 0), (stage_a, 1), (stage_a, 2), (stage_a, 3),
                 (stage_z, 0), (stage_z, 1), (stage_y, 0), (stage_c, 0))
        left_part(0)
        arrivals((stage_z, 2), (stage_y, 1))
        left_part(1)
        arrivals((stage_z, 3), (stage_y, 2), (stage_c, 1))
        left_part(2)
        arrivals((stage_y, 3), )
        left_part(3)
        arrivals((stage_c, 2), )
        left_part(4)
        left_part(5)
        arrivals((stage_c, 3), )
        left_part(6)
        left_part(7)

        @pl.when(j > 0)
        def _():
            for ch in range(NC):
                for i in range(3):
                    aa_copy(ch, i).wait_send()
                for s in sends:
                    ag_copy(ch, *s).wait_send()

        pair_phase(0)
        right_phase(0, 0, 0)
        rs_copy(0).start()
        right_phase(0, 1, 1)
        rs_copy(1).start()
        pair_phase(1)
        right_phase(1, 0, 2)
        rs_copy(2).start()
        right_phase(1, 1, 3)
        out_copy(cur, j).wait()
        for i in range(3):
            rs_copy(i).wait()

        beta_prev = bsc[0:1, 0:1]

        def pass1(p, acc):
            s1, sb, vv = acc
            w = ((sacc[3, p] + rsr[0, p]) + (rsr[1, p] + rsr[2, p]))
            v = vs[cur, p]
            sacc[3, p] = w
            return s1 + w * v, sb + (w - beta_prev * vs[prv, p]) * v, vv + v * v
        zero = jnp.zeros((16, 512), f32)
        s1, sb, vv = lax.fori_loop(0, 16, pass1, (zero, zero, zero))
        s1, sb, vv = total(s1), total(sb), total(vv)
        a_loc = jnp.where(vv > 1e-6, sb / jnp.where(vv > 1e-6, vv, 1.0), 0.0)

        def pass2(p, acc):
            uu, uv = acc
            v = vs[cur, p]
            u = sacc[3, p] - beta_prev * vs[prv, p] - a_loc * v
            return uu + u * u, uv + u * v
        uu, uv = lax.fori_loop(0, 16, pass2, (zero, zero))
        uu, uv = total(uu), total(uv)
        row = lax.broadcasted_iota(jnp.int32, (8, 128), 0)
        msg = jnp.where(row == 0, s1, jnp.where(row == 1, a_loc, jnp.where(row == 2, uu, jnp.where(row == 3, uv, vv))))
        arr[par, me] = msg

        def ar_copy(i):
            return pltpu.make_async_remote_copy(
                src_ref=arr.at[par, me], dst_ref=arr.at[par, me], send_sem=ar_send, recv_sem=ar_recv,
                device_id=(lax.rem(me + i, NDEV),), device_id_type=MESH)

        def send_msg(i, _):
            ar_copy(i).start()
            return 0
        lax.fori_loop(1, NDEV, send_msg, 0)
        pltpu.make_async_copy(arr.at[par, pl.ds(0, NDEV - 1)], arr.at[par, pl.ds(0, NDEV - 1)], ar_recv).wait()
        pltpu.make_async_copy(arr.at[par, pl.ds(0, NDEV - 1)], arr.at[par, pl.ds(0, NDEV - 1)], ar_send).wait()
        alpha = jnp.sum(arr[par, :, 0], axis=0, keepdims=True) * inv_n
        delta = alpha - arr[par, :, 1]
        rest = arr[par, :, 2] + delta * (delta * arr[par, :, 4] - 2.0 * arr[par, :, 3])
        beta = jnp.sqrt(jnp.sum(rest, axis=0, keepdims=True) * inv_n)
        alpha_ref[pl.ds(j, 1), :] = alpha
        beta_ref[pl.ds(j, 1), :] = beta
        bsc[0:1, :] = beta
        alpha11 = alpha[:, 0:1]
        beta11 = beta[:, 0:1]

        def update(p, _):
            vs[nxt, p] = (sacc[3, p] - alpha11 * vs[cur, p] - beta_prev * vs[prv, p]) / beta11
            return 0
        lax.fori_loop(0, 16, update, 0)
        out_copy(nxt, j + 1).start()

        @pl.when(j < KRYLOV_STEPS - 1)
        def _():
            for ch in range(NC):
                def fill(pp, _):
                    even = vs[nxt, 2 * pp].astype(bf16)
                    odd = vs[nxt, 2 * pp + 1].astype(bf16)
                    for r in range(4):
                        vsend[r, pp, :, 0:128] = even[:, r * 128:(r + 1) * 128]
                        vsend[r, pp, :, 128:256] = odd[:, r * 128:(r + 1) * 128]
                    vbuf[zh, zl, y, x, c, pp] = vsend[role, pp]
                    return 0
                lax.fori_loop(ch * ppc, (ch + 1) * ppc, fill, 0)
                for i in range(3):
                    aa_copy(ch, i).start()
        return 0

    lax.fori_loop(0, KRYLOV_STEPS, step, 0)
    out_copy(KRYLOV_STEPS % 3, KRYLOV_STEPS).wait()


def run_kernel(elem_count, vb0, left, wx, right, v0):
    f32, bf16 = jnp.float32, jnp.bfloat16
    vm = pl.BlockSpec(memory_space=pltpu.VMEM)
    anyspace = pl.BlockSpec(memory_space=pl.ANY)
    dma = pltpu.SemaphoreType.DMA
    return pl.pallas_call(
        functools.partial(kernel, elem_count),
        out_shape=(jax.ShapeDtypeStruct((KRYLOV_STEPS + 1, 16, 16, 512), f32),
                   jax.ShapeDtypeStruct((8, 128), f32), jax.ShapeDtypeStruct((8, 128), f32)),
        in_specs=[anyspace] * 5,
        out_specs=(anyspace, vm, vm),
        scratch_shapes=[
            pltpu.VMEM((4, 8, 4, 3, 16, 512), bf16),
            pltpu.VMEM((NT, 256, 256), bf16),
            pltpu.VMEM((NT, 128, 512), bf16),
            pltpu.VMEM((2, 2, 2, 2, 2, 8, 16, 256), bf16),
            pltpu.VMEM((4, 8, 16, 256), bf16),
            pltpu.VMEM((2, NT, 16, 16, 256), bf16),
            pltpu.VMEM((4, 16, 16, 512), f32),
            pltpu.VMEM((3, 16, 16, 512), f32),
            pltpu.VMEM((3, 16, 16, 512), f32),
            pltpu.VMEM((2, NDEV, 8, 128), f32),
            pltpu.VMEM((8, 128), f32),
            dma((8,)), dma, dma, dma((3,)), dma((3,)), dma((4, 7)), dma((4, 8)), dma, dma, dma((3,)), dma((3,)),
            dma, dma((3,)), dma((3,)), dma, dma, dma((NC, 3)), dma((NC, 3)), dma((NC, 7)), dma((NC, 8)),
        ],
        compiler_params=pltpu.CompilerParams(has_side_effects=True, vmem_limit_bytes=67043328),
    )(vb0, left, wx, right, v0)


def solution(mesh):
    def local_run(psi_init, left_env, op_pair, right_env):
        f32, bf16 = jnp.float32, jnp.bfloat16
        me = lax.axis_index('terms')
        zh, zl, y, x, c = coords(me)
        role = 2 * zl + x
        elem_count = psi_init.size
        norm = jnp.sqrt(jnp.sum(psi_init * psi_init) / elem_count)
        cols = lax.dynamic_slice_in_dim(psi_init, role * 128, 128, 3)
        vb0 = (cols / norm).astype(bf16).reshape(32, 16, 8, 2, 128)
        vb0 = vb0.transpose(0, 2, 1, 3, 4).reshape(2, 2, 2, 2, 2, 8, 16, 256)
        rows = lax.dynamic_slice_in_dim(psi_init, me * 16, 16, 0)
        v0 = (rows / norm).reshape(16, 16, 512).transpose(1, 0, 2)
        wx = jnp.broadcast_to(op_pair[:, :, :, None], (3, 16, 16, 16)).reshape(3, 16, 256)
        out, alpha, beta = run_kernel(elem_count, vb0, left_env, wx, right_env, v0)
        vecs = out.transpose(0, 2, 1, 3).reshape(KRYLOV_STEPS + 1, 16, 4, 4, 512)
        return vecs, alpha[:KRYLOV_STEPS, 0], beta[:KRYLOV_STEPS, 0]

    return jax.shard_map(local_run, mesh=mesh, in_specs=(P(), P('terms'), P('terms'), P('terms')),
                         out_specs=(P(None, 'terms'), P(), P()), check_vma=False)
```

```python
import functools

import jax
import jax.numpy as jnp
from jax import lax
from jax.experimental import pallas as pl
from jax.experimental.pallas import tpu as pltpu
from jax.sharding import PartitionSpec as P

KRYLOV_STEPS = 6
MESH = pl.DeviceIdType.MESH
NDEV = 32
NT = 96
NC = 8
GP = 16
GR = 32


def coords(me):
    z = me // 8
    return z // 2, lax.rem(z, 2), lax.rem(me // 4, 2), lax.rem(me // 2, 2), lax.rem(me, 2)


def dev_id(zh, zl, y, x, c):
    return zh * 16 + zl * 8 + y * 4 + x * 2 + c


def kernel(elem_count, vb0_ref, left_ref, wx_ref, right_ref, v0_ref, out_ref, alpha_ref, beta_ref,
           lh_ref, kr_ref, rr_ref, vbuf, vsend, xs, sacc, rsr, vs, arr, bsc,
           in_sem, w_send, w_recv, r1_send, r1_recv, rg_send, rg_recv, l1_send, l1_recv, l2_send, l2_recv,
           out_sem, rs_send, rs_recv, ar_send, ar_recv, aa_send, aa_recv, ag_send, ag_recv):
    f32, bf16 = jnp.float32, jnp.bfloat16
    me = lax.axis_index('terms')
    zh, zl, y, x, c = coords(me)
    role = 2 * zl + x
    unit = 4 * zh + 2 * y + c
    inv_n = 1.0 / elem_count
    rs_dev = [dev_id(zh, zl, y, 1 - x, c), dev_id(zh, 1 - zl, y, x, c), dev_id(zh, 1 - zl, y, 1 - x, c)]
    rs_role = [2 * zl + (1 - x), 2 * (1 - zl) + x, 2 * (1 - zl) + (1 - x), role]
    dev_z = dev_id(1 - zh, zl, y, x, c)
    dev_y = dev_id(zh, zl, 1 - y, x, c)
    dev_c = dev_id(zh, zl, y, x, 1 - c)
    kpos = 4 * unit + role
    ppc = 8 // NC

    def aa_copy(ch, i):
        pps = pl.ds(ch * ppc, ppc)
        return pltpu.make_async_remote_copy(
            src_ref=vsend.at[rs_role[i], pps], dst_ref=vbuf.at[zh, zl, y, x, c, pps],
            send_sem=aa_send.at[ch, i], recv_sem=aa_recv.at[ch, i], device_id=(rs_dev[i],), device_id_type=MESH)

    def ag_copy(ch, slot, u, dev):
        block = vbuf.at[u // 4, :, lax.rem(u // 2, 2), :, lax.rem(u, 2), pl.ds(ch * ppc, ppc)]
        return pltpu.make_async_remote_copy(
            src_ref=block, dst_ref=block,
            send_sem=ag_send.at[ch, slot], recv_sem=ag_recv.at[ch, u], device_id=(dev,), device_id_type=MESH)

    unit_z = 4 * (1 - zh) + 2 * y + c
    unit_y = 4 * zh + 2 * (1 - y) + c
    unit_zy = 4 * (1 - zh) + 2 * (1 - y) + c
    sends = [(0, unit, dev_z), (1, unit, dev_y), (2, unit_z, dev_y),
             (3, unit, dev_c), (4, unit_z, dev_c), (5, unit_y, dev_c), (6, unit_zy, dev_c)]

    def start(ch, slots):
        for s in slots:
            ag_copy(ch, *sends[s]).start()

    def recv(ch, u):
        ag_copy(ch, 0, u, dev_c).wait_recv()

    def stage_a(ch):
        for i in range(3):
            aa_copy(ch, i).wait_recv()
        start(ch, (0, 1, 3))

    def stage_z(ch):
        recv(ch, unit_z)
        start(ch, (2, 4))

    def stage_y(ch):
        recv(ch, unit_y)
        start(ch, (5,))
        recv(ch, unit_zy)
        start(ch, (6,))

    def stage_c(ch):
        for a in range(2):
            for b in range(2):
                recv(ch, 4 * a + 2 * b + (1 - c))

    def left_part(pp):
        def body(ap, _):
            rhs = vbuf[:, :, :, :, :, pp].reshape(512, 256)
            for h in range(2):
                slab = jnp.where(ap == 0, rs_role[(2, 0)[h]], rs_role[(1, 3)[h]])
                res = jnp.dot(lh_ref[slab].reshape(NT * 16, 512), rhs, preferred_element_type=f32)
                res = res.astype(bf16).reshape(NT, 16, 256)
                xs[ap, :, 2 * pp, :, h * 128:(h + 1) * 128] = res[:, :, 0:128]
                xs[ap, :, 2 * pp + 1, :, h * 128:(h + 1) * 128] = res[:, :, 128:256]
            return 0
        lax.fori_loop(0, 2, body, 0)

    def pair_phase(ap):
        def body(i, _):
            for g in range(GP):
                k = i * GP + g
                zval = jnp.dot(kr_ref[k], xs[ap, k].reshape(256, 256), preferred_element_type=f32).astype(bf16)
                xs[ap, k] = zval.reshape(16, 16, 256)
            return 0
        lax.fori_loop(0, NT // GP, body, 0)

    def right_phase(ap, h, dst):
        def piece(k0):
            lhs = jnp.concatenate([xs[ap, k0 + g].reshape(256, 256)[:, h * 128:(h + 1) * 128] for g in range(GR)], axis=1)
            rhs = rr_ref[pl.ds(k0, GR)].reshape(GR * 128, 512)
            return jnp.dot(lhs, rhs, preferred_element_type=f32).reshape(16, 16, 512)
        sacc[dst] = jnp.zeros((16, 16, 512), f32)

        def body(i, _):
            sacc[dst] += piece(i * GR)
            return 0
        lax.fori_loop(0, NT // GR, body, 0)

    def rs_copy(i):
        return pltpu.make_async_remote_copy(
            src_ref=sacc.at[i], dst_ref=rsr.at[i], send_sem=rs_send.at[i], recv_sem=rs_recv.at[i],
            device_id=(rs_dev[i],), device_id_type=MESH)

    def total(val):
        return jnp.sum(jnp.sum(val, axis=0, keepdims=True), axis=1, keepdims=True)

    def out_copy(slot, j):
        return pltpu.make_async_copy(vs.at[slot], out_ref.at[j], out_sem)

    order = [role] + rs_role[:3]

    def r_rows(u, ro):
        return pl.ds(12 * u + 3 * ro, 3)

    def r1_copy(i):
        return pltpu.make_async_remote_copy(
            src_ref=right_ref.at[:, pl.ds(pl.multiple_of(128 * rs_role[i], 128), 128)],
            dst_ref=rr_ref.at[r_rows(unit, role)],
            send_sem=r1_send.at[i], recv_sem=r1_recv.at[i], device_id=(rs_dev[i],), device_id_type=MESH)

    def rg_copy(i, slot, u, dev):
        rows = r_rows(u, order[i])
        return pltpu.make_async_remote_copy(
            src_ref=rr_ref.at[rows], dst_ref=rr_ref.at[rows],
            send_sem=rg_send.at[i, slot], recv_sem=rg_recv.at[i, u], device_id=(dev,), device_id_type=MESH)

    def l_rows(d):
        return left_ref.at[:, pl.ds(pl.multiple_of(16 * d, 16), 16)]

    def l1_copies(n):
        uzh, uy, uc = lax.rem(zh + n // 4, 2), lax.rem(y + (n // 2) % 2, 2), lax.rem(c + n % 2, 2)
        dev = dev_id(uzh, zl, uy, x, uc)
        return [pltpu.make_async_remote_copy(
            src_ref=l_rows(dev_id(uzh, r // 2, uy, r % 2, uc)), dst_ref=lh_ref.at[r, unit, role],
            send_sem=l1_send, recv_sem=l1_recv, device_id=(dev,), device_id_type=MESH) for r in range(4)]

    def l2_copy(i):
        return pltpu.make_async_remote_copy(
            src_ref=lh_ref.at[:, :, role], dst_ref=lh_ref.at[:, :, role],
            send_sem=l2_send.at[i], recv_sem=l2_recv.at[i], device_id=(rs_dev[i],), device_id_type=MESH)

    def w_copy(i):
        return pltpu.make_async_remote_copy(
            src_ref=wx_ref, dst_ref=xs.at[1, pl.ds(3 * kpos, 3), 0], send_sem=w_send, recv_sem=w_recv,
            device_id=(lax.rem(me + i, NDEV),), device_id_type=MESH)

    def local_wait(ref, sem):
        pltpu.make_async_copy(ref, ref, sem).wait()

    def gather_operators():
        own_r = pltpu.make_async_copy(
            right_ref.at[:, pl.ds(pl.multiple_of(128 * role, 128), 128)], rr_ref.at[r_rows(unit, role)], in_sem.at[2])
        own_w = pltpu.make_async_copy(wx_ref, xs.at[1, pl.ds(3 * kpos, 3), 0], in_sem.at[3])
        own_l = [pltpu.make_async_copy(l_rows(dev_id(zh, r // 2, y, r % 2, c)), lh_ref.at[r, unit, role],
                                       in_sem.at[4 + r]) for r in range(4)]
        own_r.start()
        own_w.start()
        for cp in own_l:
            cp.start()
        for i in range(3):
            r1_copy(i).start()
        for n in range(1, 8):
            for cp in l1_copies(n):
                cp.start()

        def send_w(i, _):
            w_copy(i).start()
            return 0
        lax.fori_loop(1, NDEV, send_w, 0)

        def r_start(i, slots):
            for k in slots:
                rg_copy(i, *sends[k]).start()

        def r_recv(i, u):
            rg_copy(i, 0, u, dev_c).wait_recv()

        own_r.wait()
        r_start(0, (0, 1, 3))
        for i in range(3):
            r1_copy(i).wait_recv()
            r_start(i + 1, (0, 1, 3))
        for cp in own_l:
            cp.wait()
        l1_part = lh_ref.at[:, pl.ds(0, 7), 0]
        local_wait(l1_part, l1_recv)
        for i in range(3):
            l2_copy(i).start()

        own_w.wait()
        w_part = xs.at[1, pl.ds(0, 93), 0]
        local_wait(w_part, w_recv)
        keep = lax.rem(lax.broadcasted_iota(jnp.int32, (16, 256), 1), 16) == lax.broadcasted_iota(jnp.int32, (16, 256), 0)

        def build(k, _):
            w = xs[1, k, 0].astype(f32)
            for q in range(16):
                kr_ref[k, q * 16:(q + 1) * 16, :] = jnp.where(keep, w[q:q + 1, :], 0.0).astype(bf16)
            return 0
        lax.fori_loop(0, NT, build, 0)

        for t in range(5):
            if t < 4:
                r_recv(t, unit_z)
                r_start(t, (2, 4))
                r_recv(t, unit_y)
                r_start(t, (5,))
            if t >= 1:
                r_recv(t - 1, unit_zy)
                r_start(t - 1, (6,))
        for i in range(3):
            l2_copy(i).wait_recv()
        for i in range(4):
            for a in range(2):
                for b in range(2):
                    r_recv(i, 4 * a + 2 * b + (1 - c))
        for i in range(3):
            r1_copy(i).wait_send()
            l2_copy(i).wait_send()
        local_wait(l1_part, l1_send)
        local_wait(w_part, w_send)
        for i in range(4):
            for k in sends:
                rg_copy(i, *k).wait_send()

    loads = [pltpu.make_async_copy(v0_ref, vs.at[0], in_sem.at[0]), pltpu.make_async_copy(vb0_ref, vbuf, in_sem.at[1])]
    for cp in loads:
        cp.start()
    vs[2] = jnp.zeros((16, 16, 512), f32)
    bsc[...] = jnp.zeros((8, 128), f32)
    gather_operators()
    for cp in loads:
        cp.wait()
    out_copy(0, 0).start()

    def step(j, _):
        cur = lax.rem(j, 3)
        nxt = lax.rem(j + 1, 3)
        prv = lax.rem(j + 2, 3)
        par = lax.rem(j, 2)

        def arrivals(*stages):
            @pl.when(j > 0)
            def _():
                for stage, ch in stages:
                    stage(ch)

        arrivals(*[(stage_a, ch) for ch in range(NC)], (stage_z, 0), (stage_z, 1), (stage_y, 0))
        for ch in range(NC):
            later = [(stage_z, ch + 2)] if ch + 2 < NC else []
            later += [(stage_y, ch + 1)] if ch + 1 < NC else []
            arrivals(*later, (stage_c, ch))
            left_part(ch)

        @pl.when(j > 0)
        def _():
            for ch in range(NC):
                for i in range(3):
                    aa_copy(ch, i).wait_send()
                for s in sends:
                    ag_copy(ch, *s).wait_send()

        pair_phase(0)
        right_phase(0, 0, 2)
        rs_copy(2).start()
        right_phase(0, 1, 0)
        rs_copy(0).start()
        pair_phase(1)
        right_phase(1, 0, 1)
        rs_copy(1).start()
        right_phase(1, 1, 3)
        out_copy(cur, j).wait()
        for i in range(3):
            rs_copy(i).wait()

        beta_prev = bsc[0:1, 0:1]

        def pass1(p, acc):
            s1, sb, vv = acc
            w = ((sacc[3, p] + rsr[0, p]) + (rsr[1, p] + rsr[2, p]))
            v = vs[cur, p]
            sacc[3, p] = w
            return s1 + w * v, sb + (w - beta_prev * vs[prv, p]) * v, vv + v * v
        zero = jnp.zeros((16, 512), f32)
        s1, sb, vv = lax.fori_loop(0, 16, pass1, (zero, zero, zero))
        s1, sb, vv = total(s1), total(sb), total(vv)
        a_loc = jnp.where(vv > 1e-6, sb / jnp.where(vv > 1e-6, vv, 1.0), 0.0)

        def pass2(p, acc):
            uu, uv = acc
            v = vs[cur, p]
            u = sacc[3, p] - beta_prev * vs[prv, p] - a_loc * v
            return uu + u * u, uv + u * v
        uu, uv = lax.fori_loop(0, 16, pass2, (zero, zero))
        uu, uv = total(uu), total(uv)
        row = lax.broadcasted_iota(jnp.int32, (8, 128), 0)
        msg = jnp.where(row == 0, s1, jnp.where(row == 1, a_loc, jnp.where(row == 2, uu, jnp.where(row == 3, uv, vv))))
        arr[par, me] = msg

        def ar_copy(i):
            return pltpu.make_async_remote_copy(
                src_ref=arr.at[par, me], dst_ref=arr.at[par, me], send_sem=ar_send, recv_sem=ar_recv,
                device_id=(lax.rem(me + i, NDEV),), device_id_type=MESH)

        def send_msg(i, _):
            ar_copy(i).start()
            return 0
        lax.fori_loop(1, NDEV, send_msg, 0)
        pltpu.make_async_copy(arr.at[par, pl.ds(0, NDEV - 1)], arr.at[par, pl.ds(0, NDEV - 1)], ar_recv).wait()
        pltpu.make_async_copy(arr.at[par, pl.ds(0, NDEV - 1)], arr.at[par, pl.ds(0, NDEV - 1)], ar_send).wait()
        alpha = jnp.sum(arr[par, :, 0], axis=0, keepdims=True) * inv_n
        delta = alpha - arr[par, :, 1]
        rest = arr[par, :, 2] + delta * (delta * arr[par, :, 4] - 2.0 * arr[par, :, 3])
        beta = jnp.sqrt(jnp.sum(rest, axis=0, keepdims=True) * inv_n)
        alpha_ref[pl.ds(j, 1), :] = alpha
        beta_ref[pl.ds(j, 1), :] = beta
        bsc[0:1, :] = beta
        alpha11 = alpha[:, 0:1]
        beta11 = beta[:, 0:1]

        def update(p, _):
            vs[nxt, p] = (sacc[3, p] - alpha11 * vs[cur, p] - beta_prev * vs[prv, p]) / beta11
            return 0
        lax.fori_loop(0, 16, update, 0)
        out_copy(nxt, j + 1).start()

        @pl.when(j < KRYLOV_STEPS - 1)
        def _():
            for ch in range(NC):
                def fill(pp, _):
                    even = vs[nxt, 2 * pp].astype(bf16)
                    odd = vs[nxt, 2 * pp + 1].astype(bf16)
                    for r in range(4):
                        vsend[r, pp, :, 0:128] = even[:, r * 128:(r + 1) * 128]
                        vsend[r, pp, :, 128:256] = odd[:, r * 128:(r + 1) * 128]
                    vbuf[zh, zl, y, x, c, pp] = vsend[role, pp]
                    return 0
                lax.fori_loop(ch * ppc, (ch + 1) * ppc, fill, 0)
                for i in range(3):
                    aa_copy(ch, i).start()
        return 0

    lax.fori_loop(0, KRYLOV_STEPS, step, 0)
    out_copy(KRYLOV_STEPS % 3, KRYLOV_STEPS).wait()


def run_kernel(elem_count, vb0, left, wx, right, v0):
    f32, bf16 = jnp.float32, jnp.bfloat16
    vm = pl.BlockSpec(memory_space=pltpu.VMEM)
    anyspace = pl.BlockSpec(memory_space=pl.ANY)
    dma = pltpu.SemaphoreType.DMA
    return pl.pallas_call(
        functools.partial(kernel, elem_count),
        out_shape=(jax.ShapeDtypeStruct((KRYLOV_STEPS + 1, 16, 16, 512), f32),
                   jax.ShapeDtypeStruct((8, 128), f32), jax.ShapeDtypeStruct((8, 128), f32)),
        in_specs=[anyspace] * 5,
        out_specs=(anyspace, vm, vm),
        scratch_shapes=[
            pltpu.VMEM((4, 8, 4, 3, 16, 512), bf16),
            pltpu.VMEM((NT, 256, 256), bf16),
            pltpu.VMEM((NT, 128, 512), bf16),
            pltpu.VMEM((2, 2, 2, 2, 2, 8, 16, 256), bf16),
            pltpu.VMEM((4, 8, 16, 256), bf16),
            pltpu.VMEM((2, NT, 16, 16, 256), bf16),
            pltpu.VMEM((4, 16, 16, 512), f32),
            pltpu.VMEM((3, 16, 16, 512), f32),
            pltpu.VMEM((3, 16, 16, 512), f32),
            pltpu.VMEM((2, NDEV, 8, 128), f32),
            pltpu.VMEM((8, 128), f32),
            dma((8,)), dma, dma, dma((3,)), dma((3,)), dma((4, 7)), dma((4, 8)), dma, dma, dma((3,)), dma((3,)),
            dma, dma((3,)), dma((3,)), dma, dma, dma((NC, 3)), dma((NC, 3)), dma((NC, 7)), dma((NC, 8)),
        ],
        compiler_params=pltpu.CompilerParams(has_side_effects=True, vmem_limit_bytes=67043328),
    )(vb0, left, wx, right, v0)


def solution(mesh):
    def local_run(psi_init, left_env, op_pair, right_env):
        f32, bf16 = jnp.float32, jnp.bfloat16
        me = lax.axis_index('terms')
        zh, zl, y, x, c = coords(me)
        role = 2 * zl + x
        elem_count = psi_init.size
        norm = jnp.sqrt(jnp.sum(psi_init * psi_init) / elem_count)
        cols = lax.dynamic_slice_in_dim(psi_init, role * 128, 128, 3)
        vb0 = (cols / norm).astype(bf16).reshape(32, 16, 8, 2, 128)
        vb0 = vb0.transpose(0, 2, 1, 3, 4).reshape(2, 2, 2, 2, 2, 8, 16, 256)
        rows = lax.dynamic_slice_in_dim(psi_init, me * 16, 16, 0)
        v0 = (rows / norm).reshape(16, 16, 512).transpose(1, 0, 2)
        wx = jnp.broadcast_to(op_pair[:, :, :, None], (3, 16, 16, 16)).reshape(3, 16, 256)
        out, alpha, beta = run_kernel(elem_count, vb0, left_env, wx, right_env, v0)
        vecs = out.transpose(0, 2, 1, 3).reshape(KRYLOV_STEPS + 1, 16, 4, 4, 512)
        return vecs, alpha[:KRYLOV_STEPS, 0], beta[:KRYLOV_STEPS, 0]

    return jax.shard_map(local_run, mesh=mesh, in_specs=(P(), P('terms'), P('terms'), P('terms')),
                         out_specs=(P(None, 'terms'), P(), P()), check_vma=False)
```
